128 devices in a mesh: kpt: 4 (over x, y), px: 32 (over z, core).
Axes of the slice: x: 2, y: 2, z: 16, core: 2. Of those that a mesh axis runs over, the one named last changes fastest.
The devices are a block of a 8x8x16 slice.
Arguments:
- right_side: float32 [2, 3, 4, 64, 4096], P(None, None, 'kpt', 'px'), parts along dimension 2, may hold values from -6 to 6
- material: int32 [64, 4096], P('px'), may hold values from 0 to 2
- permittivity: float32 [3], replicated, may hold values from 1 to 2
- bloch_phase: float32 [12], P('kpt'), parts along dimension 0, may hold values from -3.140625 to 3.140625
- quad_shift: float32 [2], replicated, may hold values from 0.05 to 0.6, as said below
Outputs:
- solution: float32 [2, 3, 4, 64, 4096], P(None, None, 'kpt', 'px'), parts along dimension 2
- residual: float32 [2, 3, 4, 64, 4096], P(None, None, 'kpt', 'px'), parts along dimension 2
The draws below stay inside these ranges and needn't reach their ends.
There are 4 independent parts, one for each index of `kpt`. The reference program is written for one: setup_inputs(seed, part) draws one part's arguments, and reference() takes and returns one part's arrays. A program takes and returns all parts, laid end to end along the dimension named above; an argument that names none is the same for every part. Nothing has to cross between parts.
Inputs may be any that keep to these rules, and one draw needn't show every extreme that they name: quad_shift[0] lies in 0.05 to 0.1 and quad_shift[1] in 0.3 to 0.6.
All inputs are finite; a program needn't handle non-finite values.
Results may differ from the reference program's by a relative error of at most 0.0003.
Values sent between devices are 32-bit elements; how exact they have to be, the bound alone decides.
A program may use at most 128 MiB of HBM per device.

```python
import math
import jax
import jax.numpy as jnp
from jax import lax

NG = 64
VECS = 1
ITERS = 3
MATS = 3
CELLS_YZ = 4096


def draw_right_side(key, part):
    keys = jax.random.split(jax.random.fold_in(key, 11), 4)
    shape = (2, 3, VECS, NG, CELLS_YZ)
    grid_x = jnp.arange(NG, dtype=jnp.int32).astype(jnp.float32).reshape(NG, 1)
    cells = jnp.arange(CELLS_YZ, dtype=jnp.int32).reshape(1, CELLS_YZ)
    grid_y = (cells // NG).astype(jnp.float32)
    grid_z = (cells % NG).astype(jnp.float32)
    offsets = jax.random.uniform(keys[1], (3,), minval=-math.pi, maxval=math.pi)
    wave = jnp.cos(2.0 * math.pi * grid_x / NG + offsets[0]) * jnp.cos(2.0 * math.pi * grid_y / NG + offsets[1]) * jnp.cos(2.0 * math.pi * grid_z / NG + offsets[2])
    amplitude = jax.random.normal(keys[2], (2, 3, VECS, 1, 1))
    rough = jax.random.normal(keys[0], shape)
    level = jax.random.normal(keys[3], (2, 3, VECS, 1, 1))
    field = rough + level + amplitude * wave
    return jnp.clip(field, -6.0, 6.0).astype(jnp.float32)


def draw_quad_shift(key, part):
    keys = jax.random.split(jax.random.fold_in(key, 23), 2)
    real_part = jax.random.uniform(keys[0], (), minval=0.05, maxval=0.1)
    imag_part = jax.random.uniform(keys[1], (), minval=0.3, maxval=0.6)
    return jnp.stack([real_part, imag_part]).astype(jnp.float32)


def touch_ends(entries, key, low, top_value):
    dims = entries.shape
    spot = [jax.random.randint(jax.random.fold_in(key, axis), (), 0, dims[axis]) for axis in range(len(dims))]
    entries = entries.at[tuple(spot)].set(low)
    longest = dims.index(max(dims))
    spot[longest] = (spot[longest] + 1) % dims[longest]
    return entries.at[tuple(spot)].set(top_value)


def setup_inputs(seed: int = 0, part: int = 0) -> dict:
    splits = jax.random.split(jax.random.key(seed), 6)
    part_splits = jax.random.split(jax.random.fold_in(splits[5], part), 6)
    right_side = draw_right_side(jax.random.fold_in(jax.random.fold_in(splits[5], part), 71), part)
    material = touch_ends(jax.random.randint(splits[1], (NG, CELLS_YZ), 0, MATS), jax.random.fold_in(splits[1], 1), 0, MATS - 1).astype(jnp.int32)
    permittivity = jnp.clip(jnp.exp(jax.random.uniform(splits[2], (MATS,), jnp.float32, math.log(1.0), math.log(2.0))), 1.0, 2.0)
    bloch_phase = jnp.clip(jax.random.uniform(part_splits[3], (3,), jnp.float32, -3.140625, 3.140625), -3.140625, 3.140625)
    quad_shift = draw_quad_shift(jax.random.fold_in(splits[5], 71), part)
    return dict(right_side=right_side, material=material, permittivity=permittivity, bloch_phase=bloch_phase, quad_shift=quad_shift)


PRECISE = lax.Precision.HIGHEST


def block_solve(matrix_re, matrix_im, right_re, right_im):
    blocks = matrix_re.shape[0]
    system = jnp.concatenate([jnp.concatenate([matrix_re, -matrix_im], 1), jnp.concatenate([matrix_im, matrix_re], 1)], 0)
    values = jnp.concatenate([right_re, right_im], 0)
    doubled = 2 * blocks
    for pivot_row in range(doubled - 1):
        factors = system[pivot_row + 1:, pivot_row:pivot_row + 1] / system[pivot_row, pivot_row]
        system = jnp.concatenate([system[:pivot_row + 1], system[pivot_row + 1:] - factors * system[pivot_row:pivot_row + 1]], 0)
        values = jnp.concatenate([values[:pivot_row + 1], values[pivot_row + 1:] - factors * values[pivot_row:pivot_row + 1]], 0)
    rows_out = [None] * doubled
    for pivot_row in range(doubled - 1, -1, -1):
        running = values[pivot_row]
        for later_row in range(pivot_row + 1, doubled):
            running = running - system[pivot_row, later_row] * rows_out[later_row]
        rows_out[pivot_row] = running / system[pivot_row, pivot_row]
    solved = jnp.stack(rows_out, 0)
    return solved[:blocks], solved[blocks:]


def material_scale(material, permittivity):
    scaled = jnp.zeros(material.shape, jnp.float32)
    for material_id in range(permittivity.shape[0]):
        scaled = scaled + jnp.where(material == material_id, permittivity[material_id], jnp.float32(0.0))
    return scaled


def edge_weight(length_axis, along, phase_value, at_end):
    position = jnp.arange(length_axis)
    target = length_axis - 1 if at_end else 0
    weights = jnp.where(position == target, phase_value, jnp.ones((), phase_value.dtype))
    layout = tuple(length_axis if place_dim == along else 1 for place_dim in range(4))
    return weights.reshape(layout)


def forward_step(fields, along, phase_value):
    return jnp.roll(fields, -1, along) * edge_weight(fields.shape[along], along, phase_value, True) - fields


def backward_step(fields, along, phase_value):
    return jnp.roll(fields, 1, along) * edge_weight(fields.shape[along], along, jnp.conj(phase_value), False) - fields


def curl(fields, phases):
    first = forward_step(fields[2], 2, phases[1]) - forward_step(fields[1], 3, phases[2])
    second = forward_step(fields[0], 3, phases[2]) - forward_step(fields[2], 1, phases[0])
    third = forward_step(fields[1], 1, phases[0]) - forward_step(fields[0], 2, phases[1])
    return jnp.stack([first, second, third])


def curl_adjoint(fields, phases):
    first = backward_step(fields[1], 3, phases[2]) - backward_step(fields[2], 2, phases[1])
    second = backward_step(fields[2], 1, phases[0]) - backward_step(fields[0], 3, phases[2])
    third = backward_step(fields[0], 2, phases[1]) - backward_step(fields[1], 1, phases[0])
    return jnp.stack([first, second, third])


def operate(fields, inverse_eps, permit, shift_value, phases):
    return curl_adjoint(curl(fields, phases) * inverse_eps, phases) + permit * (shift_value * fields)


def precondition(fields, angles, damping):
    grid_index = jnp.arange(NG).astype(jnp.float32)
    twists = [jnp.exp(-1j * angles[which_one] * grid_index / NG) for which_one in range(3)]
    twisted = fields * twists[0].reshape(1, 1, NG, 1, 1) * twists[1].reshape(1, 1, 1, NG, 1) * twists[2].reshape(1, 1, 1, 1, NG)
    spectrum = jnp.fft.fftn(twisted, axes=(2, 3, 4))
    differences = [jnp.exp(1j * (2.0 * math.pi * grid_index + angles[which_one]) / NG) - 1.0 for which_one in range(3)]
    differences = [differences[0].reshape(1, NG, 1, 1), differences[1].reshape(1, 1, NG, 1), differences[2].reshape(1, 1, 1, NG)]
    inner_term = jnp.conj(differences[0]) * spectrum[0] + jnp.conj(differences[1]) * spectrum[1] + jnp.conj(differences[2]) * spectrum[2]
    magnitude = sum(jnp.real(differences[which_one]) ** 2 + jnp.imag(differences[which_one]) ** 2 for which_one in range(3))
    solved = jnp.stack([(spectrum[which_one] + differences[which_one] * inner_term / damping) / (magnitude + damping) for which_one in range(3)])
    returned = jnp.fft.ifftn(solved, axes=(2, 3, 4))
    return returned * jnp.conj(twists[0]).reshape(1, 1, NG, 1, 1) * jnp.conj(twists[1]).reshape(1, 1, 1, NG, 1) * jnp.conj(twists[2]).reshape(1, 1, 1, 1, NG)


def gram(left_side, right_part):
    return jnp.einsum('cvxyz,cwxyz->vw', jnp.conj(left_side), right_part, precision=PRECISE)


def mix(fields, step_coef):
    return jnp.einsum('cvxyz,vw->cwxyz', fields, step_coef, precision=PRECISE)


def reference(right_side, material, permittivity, bloch_phase, quad_shift):
    vectors = right_side.shape[2]
    residual = (right_side[0] + 1j * right_side[1]).reshape(3, vectors, NG, NG, NG)
    permit = material_scale(material, permittivity).reshape(NG, NG, NG)
    inverse_eps = 1.0 / permit
    shift_value = quad_shift[0] + 1j * quad_shift[1]
    damping = quad_shift[0] * jnp.mean(permittivity)
    phases = [jnp.exp(1j * bloch_phase[which_one]) for which_one in range(3)]
    solution = jnp.zeros_like(residual)
    direction = precondition(residual, bloch_phase, damping)
    for iteration in range(ITERS):
        image_dir = operate(direction, inverse_eps, permit, shift_value, phases)
        gram_mat = gram(direction, image_dir)
        right_mat = gram(direction, residual)
        coef_re, coef_im = block_solve(jnp.real(gram_mat), jnp.imag(gram_mat), jnp.real(right_mat), jnp.imag(right_mat))
        step_coef = coef_re + 1j * coef_im
        solution = solution + mix(direction, step_coef)
        residual = residual - mix(image_dir, step_coef)
        if iteration < ITERS - 1:
            precond = precondition(residual, bloch_phase, damping)
            update_mat = gram(image_dir, precond)
            beta_re, beta_im = block_solve(jnp.real(gram_mat), jnp.imag(gram_mat), jnp.real(update_mat), jnp.imag(update_mat))
            direction = precond + mix(direction, -(beta_re + 1j * beta_im))
    solution_out = jnp.stack([jnp.real(solution), jnp.imag(solution)]).reshape(2, 3, vectors, NG, NG * NG).astype(jnp.float32)
    residual_out = jnp.stack([jnp.real(residual), jnp.imag(residual)]).reshape(2, 3, vectors, NG, NG * NG).astype(jnp.float32)
    return (solution_out, residual_out)
```

```python
import functools
import math

import jax
import jax.numpy as jnp
from jax import lax
from jax.experimental import pallas as pl
from jax.experimental.pallas import tpu as pltpu
from jax.sharding import PartitionSpec as P

MESH = pl.DeviceIdType.MESH
NG = 64
HALF = NG // 2
LANES = 2 * NG
ITERS = 3
F32 = jnp.float32
BF16 = jnp.bfloat16


def iota(shape, dim):
    return lax.broadcasted_iota(jnp.int32, shape, dim)


def split(value):
    high = value.astype(BF16)
    return high, (value - high.astype(F32)).astype(BF16)


def turn(index, other, phase, quarter):
    whole = ((index * other) & (NG - 1)).astype(F32) * (2.0 * math.pi / NG)
    return whole + index.astype(F32) * (phase / NG) + quarter.astype(F32) * (0.5 * math.pi)


def z_table(phase, inverse):
    shape = (LANES, 2 * LANES)
    row, col = iota(shape, 0), iota(shape, 1)
    place = col if inverse else row
    angle = turn(place & (NG - 1), (row if inverse else col) & (NG - 1), phase, 0 * row)
    row_part, col_part, second = row >> 6, (col >> 6) & 1, col >> 7
    quarter = (row_part - col_part if inverse else col_part - row_part) + second
    table = jnp.cos(angle + quarter.astype(F32) * (0.5 * math.pi))
    high, low = split(table / NG if inverse else table)
    return jnp.concatenate([high, high, low], 0)


def y_table(phase, inverse):
    shape = (NG, LANES)
    row, col = iota(shape, 0), iota(shape, 1)
    grid_row, mode = (row, col & (NG - 1)) if inverse else (col & (NG - 1), row)
    place = 2 * (grid_row & (HALF - 1)) + (grid_row >> 5)
    table = jnp.cos(turn(place, mode, phase, -(col >> 6)))
    high, low = split(table / NG if inverse else table)
    return jnp.concatenate([high, high, low], 1)


def transform(tiles, z_ref, y_ref):
    high, low = split(jnp.concatenate(tiles, 0))
    mid = jnp.dot(jnp.concatenate([high, low, high], 1), z_ref[...], preferred_element_type=F32)
    done = []
    for start in range(0, len(tiles), 2):
        stacks = []
        for which in range(start, min(start + 2, len(tiles))):
            part = mid[which * NG : (which + 1) * NG]
            stacks.append(jnp.concatenate([part[:, :LANES], part[:, LANES:]], 0))
        high, low = split(jnp.concatenate(stacks, 1) if len(stacks) > 1 else stacks[0])
        out = jnp.dot(y_ref[...], jnp.concatenate([high, low, high], 0), preferred_element_type=F32)
        done += [out[:, n * LANES : (n + 1) * LANES] for n in range(len(stacks))]
    return done


def swap(value):
    return pltpu.roll(value, NG, 1)


def complex_divide(top, bottom):
    a, b = bottom
    factor = b / a
    second = (top[1] - factor * top[0]) / (a + factor * b)
    return ((top[0] + b * second) / a, second)


def cmul(x, y):
    return (x[0] * y[0] - x[1] * y[1], x[0] * y[1] + x[1] * y[0])


def cadd(x, y):
    return (x[0] + y[0], x[1] + y[1])


def csub(x, y):
    return (x[0] - y[0], x[1] - y[1])


def conj(x):
    return (x[0], -x[1])


def csum(terms):
    return functools.reduce(cadd, terms)


def steps(moments, sides, shifts):
    zero = (jnp.zeros_like(sides[0][0]),) * 2
    one = (jnp.ones_like(sides[0][0]), zero[0])

    def image(vector):
        return [csum([cmul(moments[i][j], vector[j]) for j in range(ITERS)]) for i in range(ITERS)]

    def inner(left, right):
        return csum([cmul(conj(x), y) for x, y in zip(left, right)])

    def negative(x):
        return (-x[0], -x[1])

    direction = [one, zero, zero]
    place = [zero, zero, zero]
    for step in range(ITERS):
        gram = inner(direction, image(direction))
        right = inner(direction, [csub(g, m) for g, m in zip(sides, image(place))])
        coef = complex_divide(right, gram)
        place = [cadd(p, cmul(d, coef)) for p, d in zip(place, direction)]
        if step < ITERS - 1:
            fresh = [
                csub(one, cmul(place[0], shifts[0])),
                negative(cadd(place[0], cmul(place[1], shifts[1]))),
                negative(place[1]),
            ]
            update = csum(
                [
                    cmul(conj(cmul(moments[j][i], direction[i])), fresh[j])
                    for i in range(ITERS)
                    for j in range(ITERS)
                ]
            )
            beta = complex_divide(update, gram)
            direction = [csub(z, cmul(d, beta)) for z, d in zip(fresh, direction)]
    return place


def kernel(
    count,
    b_ref, mat_ref, eps_ref, phase_ref, quad_ref,
    x_ref, res_ref,
    zf, yf, zi, yi,
    r_ref, c_ref, ie_ref, pe_ref, matlow,
    b_in, f_in, v_all, y_all,
    local, other, send1, recv1, send2, recv2, send3, carry,
    sums, gsend, grecv,
    d1s, d1r, a1s, a1r, a2s, a2r, d2s, d2r, ms, mr, gs, gr,
):
    chips = count // 2
    me = lax.axis_index("px")
    chip, core = me // 2, me % 2
    partner = me + 1 - 2 * core

    barrier = pltpu.get_barrier_semaphore()

    def greet(offset, none):
        pl.semaphore_signal(
            barrier, inc=1, device_id={"px": (me + offset) % count}, device_id_type=MESH
        )
        return none

    lax.fori_loop(1, count, greet, 0)

    lane_row = iota((1, LANES), 1)
    low_half = lane_row < NG
    sign = jnp.where(low_half, -1.0, 1.0).astype(F32)

    for comp in range(3):
        for plane in range(2):
            re = b_ref[0, comp, pl.ds(plane, HALF, 2), :]
            im = b_ref[1, comp, pl.ds(plane, HALF, 2), :]
            tile = jnp.concatenate(
                [jnp.where(low_half, re, swap(im)), jnp.where(low_half, swap(re), im)], 0
            )
            b_in[comp, plane] = tile
            f_in[comp, plane] = tile

    zf[...] = z_table(phase_ref[2], False)
    yf[...] = y_table(phase_ref[1], False)

    delta = quad_ref[0] * ((eps_ref[0] + eps_ref[1] + eps_ref[2]) * F32(1.0 / 3.0))

    def symbol(modes_y):
        half_y = (2.0 * math.pi * modes_y.astype(F32) + phase_ref[1]) * (0.5 / NG)
        half_z = (2.0 * math.pi * (lane_row & (NG - 1)).astype(F32) + phase_ref[2]) * (0.5 / NG)
        sin_y, sin_z = jnp.sin(half_y), jnp.sin(half_z)
        total = 4.0 * sin_y * sin_y + 4.0 * sin_z * sin_z + delta
        root = jnp.sqrt(total + 0.25 * total * total)
        return 1.0 / (1.0 + 0.5 * total + root), 0.5 / root

    ratio, scale = symbol(iota((NG, LANES), 0))
    r_ref[...] = ratio
    c_ref[...] = scale

    own_ratio, _ = symbol(iota((4, LANES), 0) + 4 * chip)
    decay = own_ratio * own_ratio
    decay = decay * decay
    around = decay
    for _ in range(4):
        around = around * around
    turn_x = jnp.full((1, LANES), phase_ref[0], F32)
    cos_x, sin_x = jnp.cos(turn_x), jnp.sin(turn_x)
    under = 1.0 - 2.0 * around * cos_x + around * around
    wrap_re = (cos_x - around) / under
    wrap_im = sign * ((2 * core - 1).astype(F32) * sin_x) / under

    pl.semaphore_wait(barrier, count - 1)

    above = (me + 1) % count
    lower = pltpu.make_async_remote_copy(
        src_ref=mat_ref, dst_ref=matlow, send_sem=ms, recv_sem=mr,
        device_id={"px": above}, device_id_type=MESH,
    )
    lower.start()

    zi[...] = z_table(phase_ref[2], True)
    yi[...] = y_table(phase_ref[1], True)

    def permit_of(ref, plane):
        kind = ref[pl.ds(plane, HALF, 2), :]
        value = jnp.zeros(kind.shape, F32)
        for which in range(3):
            value = value + jnp.where(kind == which, eps_ref[which], F32(0.0))
        return jnp.concatenate(
            [jnp.where(low_half, value, swap(value)), jnp.where(low_half, swap(value), value)], 0
        )

    for plane in range(2):
        permit = permit_of(mat_ref, plane)
        pe_ref[plane] = permit
        ie_ref[plane + 1] = 1.0 / permit
    lower.wait()
    ie_ref[0] = 1.0 / permit_of(matlow, 1)

    def vec(scalar):
        return jnp.full((1, LANES), scalar, F32)

    modes_y = iota((NG, LANES), 0).astype(F32)
    half_y = (2.0 * math.pi * modes_y + phase_ref[1]) * (0.5 / NG)
    half_z = (2.0 * math.pi * (lane_row & (NG - 1)).astype(F32) + phase_ref[2]) * (0.5 / NG)

    cos_y, sin_y = jnp.cos(vec(phase_ref[1])), jnp.sin(vec(phase_ref[1]))
    cos_z, sin_z = jnp.cos(vec(phase_ref[2])), jnp.sin(vec(phase_ref[2]))
    last_z, first_z = (lane_row & (NG - 1)) == NG - 1, (lane_row & (NG - 1)) == 0
    up_a = jnp.where(last_z, sign * sin_z, 1.0)
    up_b = jnp.where(last_z, cos_z, 0.0)
    down_a = jnp.where(first_z, -sign * sin_z, 1.0)
    down_b = jnp.where(first_z, cos_z, 0.0)

    def dz_up(tile):
        return (
            pltpu.roll(tile, LANES - 1, 1) * up_a + pltpu.roll(tile, NG - 1, 1) * up_b - tile
        )

    def dz_down(tile):
        return pltpu.roll(tile, 1, 1) * down_a + pltpu.roll(tile, NG + 1, 1) * down_b - tile

    def dy_up(tile):
        even, odd = tile[:HALF], tile[HALF:]
        edge = even[:1]
        edge = cos_y * edge + sin_y * (sign * swap(edge))
        return jnp.concatenate([odd, even[1:], edge], 0) - tile

    def dy_down(tile):
        even, odd = tile[:HALF], tile[HALF:]
        edge = odd[HALF - 1 :]
        edge = cos_y * edge - sin_y * (sign * swap(edge))
        return jnp.concatenate([edge, odd[: HALF - 1], even], 0) - tile

    shift_im = quad_ref[1] / quad_ref[0]

    order = [chips // 2]
    for gap in range(chips // 2 - 1, 0, -1):
        order += [gap, chips - gap]

    def spread(it, source, target, send_sem, recv_sem):
        for offset in order:
            there = (chip + offset) % chips
            pltpu.make_async_remote_copy(
                src_ref=source.at[it, there],
                dst_ref=target.at[it, chip],
                send_sem=send_sem.at[it],
                recv_sem=recv_sem.at[it],
                device_id={"px": 2 * there + core},
                device_id_type=MESH,
            ).start()

    def drained(buffer, it, sem):
        some = buffer.at[it, pl.ds(0, chips - 1)]
        pltpu.make_async_copy(some, some, sem.at[it]).wait()

    def iteration(it, none):
        modes = transform([f_in[c, p] for c in range(3) for p in range(2)], zf, yf)
        ratio = r_ref[...]
        for comp in range(3):
            near, far = modes[2 * comp], modes[2 * comp + 1]
            local[it, 0, comp] = far + ratio * near
            local[it, 1, comp] = near + ratio * far
        across = pltpu.make_async_remote_copy(
            src_ref=local.at[it, 1 - core], dst_ref=other.at[it],
            send_sem=d1s.at[it], recv_sem=d1r.at[it],
            device_id={"px": partner}, device_id_type=MESH,
        )
        across.start()
        across.wait_recv()
        square = ratio * ratio
        for comp in range(3):
            whole = other[it, comp] + square * local[it, core, comp]
            for piece in range(chips):
                send1[it, piece, comp] = whole[4 * piece : 4 * piece + 4]
        spread(it, send1, recv1, a1s, a1r)
        recv1[it, chip] = send1[it, chip]
        drained(recv1, it, a1r)

        spots = [step + core * (chips - 1 - 2 * step) for step in range(chips)]
        items = [recv1[it, spot] for spot in spots]
        wide = decay[None]
        total = items[0]
        for item in items[1:]:
            total = wide * total + item
        swapped = pltpu.roll(total, NG, 2)
        inside = wrap_re[None] * total + wrap_im[None] * swapped
        for spot, item in zip(spots, items):
            send2[it, spot] = inside
            inside = wide * inside + item
        spread(it, send2, recv2, a2s, a2r)
        recv2[it, chip] = send2[it, chip]
        drained(recv2, it, a2r)

        for comp in range(3):
            for piece in range(chips):
                carry[it, core, comp, 4 * piece : 4 * piece + 4, :] = recv2[it, piece, comp]
        for comp in range(3):
            send3[it, comp] = local[it, core, comp] + square * carry[it, core, comp]
        back = pltpu.make_async_remote_copy(
            src_ref=send3.at[it], dst_ref=carry.at[it, core],
            send_sem=d2s.at[it], recv_sem=d2r.at[it],
            device_id={"px": partner}, device_id_type=MESH,
        )
        back.start()
        back.wait_recv()

        waves = []
        scale = c_ref[...]
        for comp in range(3):
            from_low, from_high = carry[it, 0, comp], carry[it, 1, comp]
            up = local[it, 0, comp] + square * from_low
            down = local[it, 1, comp] + square * from_high
            waves.append(
                [
                    scale * (from_low + ratio * down),
                    scale * (ratio * from_low + down),
                    scale * (up + ratio * from_high),
                    scale * (ratio * up + from_high),
                ]
            )
        sy, cy = jnp.sin(half_y), jnp.cos(half_y)
        sz, cz = jnp.sin(half_z), jnp.cos(half_z)
        dyr, dyi = -2.0 * sy * sy, (2.0 * sy * cy) * sign
        dzr, dzi = -2.0 * sz * sz, (2.0 * sz * cz) * sign
        inverse_delta = 1.0 / vec(delta)
        phi = []
        for j in range(3):
            w_y, w_z = waves[1][j + 1], waves[2][j + 1]
            gap = waves[0][j] - waves[0][j + 1] + (dyr * w_y + dzr * w_z)
            phi.append((gap - (dyi * swap(w_y) + dzi * swap(w_z))) * inverse_delta)
        spun = [swap(p) for p in phi]
        tiles = [
            waves[0][0] + phi[0],
            waves[0][1] + (phi[1] - phi[0]),
            waves[0][2] + (phi[2] - phi[1]),
            waves[1][0],
        ]
        tiles += [waves[1][j + 1] + dyr * phi[j] + dyi * spun[j] for j in range(3)]
        tiles += [waves[2][0]]
        tiles += [waves[2][j + 1] + dzr * phi[j] + dzi * spun[j] for j in range(3)]
        real = transform(tiles, zi, yi)
        ex, ey, ez = real[:3], real[3:7], real[7:]

        gx, gy, gz = [None] * 3, [None] * 3, [None] * 3
        for j in range(3):
            inv = ie_ref[j]
            if j > 0:
                gx[j] = inv * (dy_up(ez[j]) - dz_up(ey[j]))
            gy[j] = inv * (dz_up(ex[j]) - (ez[j + 1] - ez[j]))
            gz[j] = inv * ((ey[j + 1] - ey[j]) - dy_up(ex[j]))
        theta_re = jnp.where(it == 0, F32(0.8), F32(0.7))
        theta_im = jnp.where(it == 0, shift_im, F32(0.0))
        for plane in range(2):
            j = plane + 1
            permit = pe_ref[plane]
            fields = (ex[j], ey[j], ez[j])
            curls = (
                dz_down(gy[j]) - dy_down(gz[j]),
                (gz[j - 1] - gz[j]) - dz_down(gx[j]),
                dy_down(gx[j]) - (gy[j - 1] - gy[j]),
            )
            for comp in range(3):
                e = fields[comp]
                y = curls[comp] + permit * (quad_ref[0] * e + quad_ref[1] * (sign * swap(e)))
                v_all[it, comp, plane] = e
                y_all[it, comp, plane] = y
                f = f_in[comp, plane]
                f_in[comp, plane] = y - (theta_re * f + theta_im * (sign * swap(f)))

        across.wait_send()
        drained(send1, it, a1s)
        drained(send2, it, a2s)
        back.wait_send()
        return none

    lax.fori_loop(0, ITERS, iteration, 0)

    pairs = [(i, j) for i in range(ITERS) for j in range(ITERS + 1)]
    plain = [jnp.zeros((8, LANES), F32) for _ in pairs]
    crossed = [jnp.zeros((8, LANES), F32) for _ in pairs]

    def folded(value):
        return jnp.sum(value.reshape(NG // 8, 8, LANES), 0)

    for comp in range(3):
        for plane in range(2):
            lefts = [v_all[i, comp, plane] for i in range(ITERS)]
            for j in range(ITERS + 1):
                right = y_all[j, comp, plane] if j < ITERS else b_in[comp, plane]
                around_z = swap(right)
                for i in range(ITERS):
                    at = i * (ITERS + 1) + j
                    plain[at] = plain[at] + folded(lefts[i] * right)
                    crossed[at] = crossed[at] + folded(lefts[i] * around_z)
    for at in range(len(pairs)):
        sums[2 * at : 2 * at + 1, :] = jnp.sum(plain[at], 0, keepdims=True)
        sums[2 * at + 1 : 2 * at + 2, :] = jnp.sum(-sign * crossed[at], 0, keepdims=True)
    wide = (2 * len(pairs), LANES)
    totals = jnp.sum(sums[...], 1, keepdims=True)
    row = jnp.sum(jnp.where(iota(wide, 0) == iota(wide, 1), totals, 0.0), 0, keepdims=True)
    gsend[0] = row
    grecv[me] = row

    def tell(offset, none):
        pltpu.make_async_remote_copy(
            src_ref=gsend.at[0], dst_ref=grecv.at[me], send_sem=gs, recv_sem=gr,
            device_id={"px": (me + offset) % count}, device_id_type=MESH,
        ).start()
        return none

    lax.fori_loop(1, count, tell, 0)
    rest = grecv.at[pl.ds(0, count - 1)]
    pltpu.make_async_copy(rest, rest, gr).wait()
    row = jnp.sum(grecv[...], 0)
    spread_out = jnp.where(iota(wide, 0) == iota(wide, 1), jnp.broadcast_to(row, wide), 0.0)
    sums[...] = jnp.broadcast_to(jnp.sum(spread_out, 1, keepdims=True), wide)

    def number(at):
        return (sums[2 * at : 2 * at + 1, :], sums[2 * at + 1 : 2 * at + 2, :])

    moments = [[number(i * (ITERS + 1) + j) for j in range(ITERS)] for i in range(ITERS)]
    sides = [number(i * (ITERS + 1) + ITERS) for i in range(ITERS)]
    shifts = [(vec(0.8), vec(shift_im)), (vec(0.7), vec(0.0))]
    coefs = steps(moments, sides, shifts)

    for comp in range(3):
        for plane in range(2):
            for kept, ref, base in ((v_all, x_ref, None), (y_all, res_ref, b_in)):
                parts = [kept[i, comp, plane] for i in range(ITERS)]
                direct = sum(coefs[i][0] * parts[i] for i in range(ITERS))
                twisted = sum(coefs[i][1] * parts[i] for i in range(ITERS))
                tile = direct + sign * swap(twisted)
                if base is not None:
                    tile = base[comp, plane] - tile
                even, odd = tile[:HALF], tile[HALF:]
                ref[0, comp, pl.ds(plane, HALF, 2), :] = jnp.where(low_half, even, swap(odd))
                ref[1, comp, pl.ds(plane, HALF, 2), :] = jnp.where(low_half, swap(even), odd)

    everything = grecv.at[pl.ds(0, count - 1)]
    pltpu.make_async_copy(everything, everything, gs).wait()


def on_device(right_side, material, permittivity, bloch_phase, quad_shift):
    count = lax.axis_size("px")
    chips = count // 2
    shape = right_side.shape
    b = right_side.reshape(2, 3, 2, HALF, LANES).swapaxes(2, 3).reshape(2, 3, NG, LANES)
    mat = material.reshape(2, HALF, LANES).swapaxes(0, 1).reshape(NG, LANES)
    tile = (NG, LANES)
    vmem = pl.BlockSpec(memory_space=pltpu.VMEM)
    smem = pl.BlockSpec(memory_space=pltpu.SMEM)
    pieces = pltpu.VMEM((ITERS, chips, 3, 4, LANES), F32)
    dma = pltpu.SemaphoreType.DMA
    out = jax.ShapeDtypeStruct((2, 3, NG, LANES), F32)
    found, left = pl.pallas_call(
        functools.partial(kernel, count),
        out_shape=(out, out),
        in_specs=[vmem, vmem, smem, smem, smem],
        out_specs=(vmem, vmem),
        scratch_shapes=[
            pltpu.VMEM((3 * LANES, 2 * LANES), BF16),
            pltpu.VMEM((NG, 3 * LANES), BF16),
            pltpu.VMEM((3 * LANES, 2 * LANES), BF16),
            pltpu.VMEM((NG, 3 * LANES), BF16),
            pltpu.VMEM(tile, F32),
            pltpu.VMEM(tile, F32),
            pltpu.VMEM((3, *tile), F32),
            pltpu.VMEM((2, *tile), F32),
            pltpu.VMEM(tile, jnp.int32),
            pltpu.VMEM((3, 2, *tile), F32),
            pltpu.VMEM((3, 2, *tile), F32),
            pltpu.VMEM((ITERS, 3, 2, *tile), F32),
            pltpu.VMEM((ITERS, 3, 2, *tile), F32),
            pltpu.VMEM((ITERS, 2, 3, *tile), F32),
            pltpu.VMEM((ITERS, 3, *tile), F32),
            pieces,
            pieces,
            pieces,
            pieces,
            pltpu.VMEM((ITERS, 3, *tile), F32),
            pltpu.VMEM((ITERS, 2, 3, *tile), F32),
            pltpu.VMEM((2 * ITERS * (ITERS + 1), LANES), F32),
            pltpu.VMEM((1, 1, LANES), F32),
            pltpu.VMEM((count, 1, LANES), F32),
            *[dma((ITERS,)) for _ in range(8)],
            *[dma for _ in range(4)],
        ],
        compiler_params=pltpu.CompilerParams(
            collective_id=0, has_side_effects=True, vmem_limit_bytes=40 * 1024 * 1024
        ),
    )(b, mat, permittivity, bloch_phase, quad_shift)

    def back(value):
        return value.reshape(2, 3, HALF, 2, LANES).swapaxes(2, 3).reshape(shape)

    return back(found), back(left)


def solution(mesh):
    in_specs = (P(None, None, "kpt", "px", None), P("px", None), P(), P("kpt"), P())
    out_specs = (P(None, None, "kpt", "px", None), P(None, None, "kpt", "px", None))
    return jax.shard_map(
        on_device, mesh=mesh, in_specs=in_specs, out_specs=out_specs, check_vma=False
    )
```
